256 devices in a mesh: dp: 4 (over x_hi, core), centre: 64 (over z, y, x_lo).
Axes of the slice: x: 4 (x_hi: 2, x_lo: 2; x = x_hi * 2 + x_lo), y: 4, z: 8, core: 2. Of those that a mesh axis runs over, the one named last changes fastest.
Arguments:
- samples: bfloat16 [16384, 128], P('dp'), may hold values from -24 to 24
- centres: bfloat16 [16384, 128], P('centre'), may hold values from -6 to 6
- facility_prior_logprob: float32 [16384], P('centre'), may hold values from -2 to 0
Outputs:
- new_centres: float32 [16384, 128], P('centre')
- new_log_prior: float32 [16384], P('centre')
- log_partition: float32 [16384], P('dp')
The draws below stay inside these ranges and needn't reach their ends.
All inputs are finite; a program needn't handle non-finite values.
Results may differ from the reference program's by a relative error of at most 0.00075.
Values sent between devices are 32-bit elements; how exact they have to be, the bound alone decides.
No kernel may reach another device: no remote copies, remote signals or barrier semaphores. Data moves between devices by JAX's collectives and lax.ppermute only.
A program may use at most 64 MiB of HBM per device.

```python
import jax
import jax.numpy as jnp
from jax import lax

F = 128
K = 16384
NS = 16384


def draw_samples(key, part):
    first = jax.random.fold_in(key, 0)
    fourth = jax.random.fold_in(key, 71)
    fifth = jax.random.fold_in(key, 83)
    values = jax.random.normal(first, (NS, F), jnp.float32)
    reach = jax.random.uniform(fourth, (NS, 1), jnp.float32, 3500.0, 6000.0)
    shift_size = jnp.sqrt(reach / float(F))
    signs = jnp.where(jax.random.uniform(fifth, (NS, 1), jnp.float32) < 0.5, -1.0, 1.0)
    row_index = lax.broadcasted_iota(jnp.int32, (NS, 1), 0)
    far_rows = row_index % 2 == 1
    shifted = jnp.where(far_rows, values + signs * shift_size, values)
    return jnp.clip(shifted, -24.0, 24.0).astype(jnp.bfloat16)


def block_levels(own_key, dims, cuts, least, high):
    loudness, own = 1.0, jax.random.fold_in(own_key, 6)
    for position, shards_of in cuts:
        heights = jnp.exp(jax.random.uniform(jax.random.fold_in(own, position), (shards_of,), jnp.float32, least / len(cuts), high / len(cuts)))
        loudness = loudness * jnp.repeat(heights, dims[position] // shards_of).reshape([-1 if axis == position else 1 for axis in range(len(dims))])
    return loudness


def gaussian(stream_key, dims, spread, limit, shards=(), dtype=jnp.bfloat16):
    gain = block_levels(stream_key, dims, shards, -0.22, 0.18) if shards else 1.0
    array = jax.random.normal(stream_key, dims, jnp.float32) * spread * gain
    return jnp.minimum(jnp.maximum(array, -limit), limit).astype(dtype)


def setup_inputs(seed: int = 0) -> dict:
    streams_of = jax.random.split(jax.random.key(seed), 4)
    samples = draw_samples(jax.random.fold_in(streams_of[3], 71), 0)
    centres = gaussian(streams_of[1], (K, F), 1.0, 6.0, ((0, 64),))
    facility_prior_logprob = jnp.clip(-2.0 + 2.0 * jax.random.uniform(streams_of[2], (K,), jnp.float32) ** block_levels(streams_of[2], (K,), ((0, 64),), -0.2, 0.2), -2.0, 0.0)
    return {"samples": samples, "centres": centres, "facility_prior_logprob": facility_prior_logprob}


inverse_coolness_beta = 0.0625


def reference(samples, centres, facility_prior_logprob):
    centres_wide = centres.astype(jnp.float32)
    facility_norm_sq = jnp.sum(centres_wide * centres_wide, axis=1)
    block_rows = min(512, NS)
    blocks = samples.reshape(NS // block_rows, block_rows, F)

    def block_step(running, rows_block):
        mass, weighted = running
        padded_row_width = rows_block.astype(jnp.float32)
        point_norm_sq = jnp.sum(padded_row_width * padded_row_width, axis=1)
        point_facility_inner = jnp.dot(rows_block, centres.T, preferred_element_type=jnp.float32)
        unnormalised_membership_energy = facility_prior_logprob[None, :] - (point_norm_sq[:, None] - 2.0 * point_facility_inner + facility_norm_sq[None, :]) * inverse_coolness_beta
        row_max = jnp.max(unnormalised_membership_energy, axis=1)
        row_total = jnp.sum(jnp.exp(unnormalised_membership_energy - row_max[:, None]), axis=1)
        partition = row_max + jnp.log(row_total)
        resp = jnp.exp(unnormalised_membership_energy - partition[:, None]).astype(jnp.bfloat16)
        mass = mass + jnp.sum(resp.astype(jnp.float32), axis=0)
        weighted = weighted + jnp.dot(resp.T, rows_block, preferred_element_type=jnp.float32)
        return (mass, weighted), partition

    start = (jnp.zeros((K,), jnp.float32), jnp.zeros((K, F), jnp.float32))
    (mass, weighted), partitions = lax.scan(block_step, start, blocks)
    new_centres = (weighted + centres_wide) / (mass + 1.0)[:, None]
    new_log_prior = jnp.log((mass + 1.0) / float(NS + K))
    return new_centres, new_log_prior, partitions.reshape(NS)
```

```python
import jax
import jax.numpy as jnp
import numpy as np
from jax import lax
from jax.experimental import pallas as pl
from jax.experimental.pallas import tpu as pltpu
from jax.sharding import Mesh
from jax.sharding import PartitionSpec as P

AXES = ("xh", "core", "z", "y", "xl")
DP = ("xh", "core")
CENTRE = ("z", "y", "xl")

inverse_coolness_beta = 0.0625
LOG2E = float(np.log2(np.e))
LN2 = float(np.log(2.0))
CROSS2 = 2.0 * inverse_coolness_beta * LOG2E

LANES = 128
TILE = 256


def column_of(row):
    return jnp.transpose(jnp.broadcast_to(row, (LANES, LANES)))


def centre_bias(centres_ref, prior_ref):
    wide = centres_ref[...].astype(jnp.float32)
    norm = jnp.sum(wide * wide, axis=1, keepdims=True)
    prior = jnp.concatenate([column_of(prior_ref[k : k + 1, :]) for k in range(prior_ref.shape[0])])
    return (prior - norm * inverse_coolness_beta) * LOG2E


def cross_tile(centres_ref, rows):
    return lax.dot_general(
        centres_ref[...], rows, (((1,), (1,)), ((), ())), preferred_element_type=jnp.float32
    )


def stats_kernel(samples_ref, centres_ref, prior_ref, out_ref):
    bias = centre_bias(centres_ref, prior_ref)
    for t in range(samples_ref.shape[0] // TILE):
        cross = cross_tile(centres_ref, samples_ref[t * TILE : (t + 1) * TILE, :])
        for h in range(TILE // LANES):
            score = cross[:, h * LANES : (h + 1) * LANES] * CROSS2 + bias
            top = jnp.max(score, axis=0, keepdims=True)
            total = jnp.sum(jnp.exp2(score - top), axis=0, keepdims=True)
            at = t * (TILE // LANES) + h
            out_ref[at : at + 1, :] = top + jnp.log2(total)


def accumulate_kernel(samples_ref, centres_ref, prior_ref, partition_ref, out_ref):
    bias = centre_bias(centres_ref, prior_ref)
    local = centres_ref.shape[0]
    weighted = jnp.zeros((local, LANES), jnp.float32)
    mass = jnp.zeros((local, LANES), jnp.float32)
    for t in range(samples_ref.shape[0] // TILE):
        rows = samples_ref[t * TILE : (t + 1) * TILE, :]
        cross = cross_tile(centres_ref, rows)
        for h in range(TILE // LANES):
            at = t * (TILE // LANES) + h
            score = cross[:, h * LANES : (h + 1) * LANES] * CROSS2 + bias
            resp = jnp.exp2(score - partition_ref[at : at + 1, :]).astype(jnp.bfloat16)
            mass = mass + resp.astype(jnp.float32)
            weighted = weighted + lax.dot_general(
                resp,
                rows[h * LANES : (h + 1) * LANES, :],
                (((1,), (0,)), ((), ())),
                preferred_element_type=jnp.float32,
            )
    out_ref[0:local, :] = weighted
    out_ref[local:, :] = jnp.zeros((out_ref.shape[0] - local, LANES), jnp.float32)
    for k in range(local // LANES):
        block = jnp.transpose(mass[k * LANES : (k + 1) * LANES, :])
        out_ref[local + k : local + k + 1, :] = jnp.sum(block, axis=0, keepdims=True)


def finish_kernel(denominator, mine_ref, other_ref, centres_ref, new_ref, prior_ref):
    local = centres_ref.shape[0]
    for k in range(local // LANES):
        rows = slice(k * LANES, (k + 1) * LANES)
        at = slice(local + k, local + k + 1)
        mass = mine_ref[at, :] + other_ref[at, :] + 1.0
        prior_ref[k : k + 1, :] = jnp.log(mass / denominator)
        weighted = mine_ref[rows, :] + other_ref[rows, :]
        new_ref[rows, :] = (weighted + centres_ref[rows, :].astype(jnp.float32)) / column_of(mass)


def shared(x, axes):
    n = lax.axis_size(axes)
    return lax.all_to_all(jnp.broadcast_to(x, (n, *x.shape)), axes, 0, 0, tiled=True)


def merged(parts):
    top = jnp.max(parts, axis=0)
    return top + jnp.log2(jnp.sum(jnp.exp2(parts - top), axis=0))


def swapped(x, axis):
    return lax.ppermute(x, axis, [(0, 1), (1, 0)])


def shards(samples, centres, facility_prior_logprob):
    rows, features = samples.shape
    local = centres.shape[0]
    prior = facility_prior_logprob.reshape(local // LANES, LANES)
    partition = pl.pallas_call(
        stats_kernel, out_shape=jax.ShapeDtypeStruct((rows // LANES, LANES), jnp.float32)
    )(samples, centres, prior)
    partition = merged(shared(partition, ("y", "xl")))
    partition = merged(shared(partition, "z"))
    sums = pl.pallas_call(
        accumulate_kernel, out_shape=jax.ShapeDtypeStruct((local + 8, features), jnp.float32)
    )(samples, centres, prior, partition)
    sums = sums + swapped(sums, "core")
    other = swapped(sums, "xh")
    wide = samples.astype(jnp.float32)
    norms = jnp.sum(wide * wide, axis=1)
    log_partition = partition.reshape(rows) * LN2 - norms * inverse_coolness_beta
    denominator = float(rows * lax.axis_size(DP) + local * lax.axis_size(CENTRE))
    new_centres, new_log_prior = pl.pallas_call(
        lambda *refs: finish_kernel(denominator, *refs),
        out_shape=(
            jax.ShapeDtypeStruct((local, features), jnp.float32),
            jax.ShapeDtypeStruct((local // LANES, LANES), jnp.float32),
        ),
    )(sums, other, centres)
    return new_centres, new_log_prior.reshape(local), log_partition


def solution(mesh):
    torus = Mesh(mesh.devices.reshape(2, 2, 8, 4, 2), AXES)
    in_specs = (P(DP, None), P(CENTRE, None), P(CENTRE))
    out_specs = (P(CENTRE, None), P(CENTRE), P(DP))
    return jax.shard_map(
        shards, mesh=torus, in_specs=in_specs, out_specs=out_specs, check_vma=False
    )
```

```python
import jax
import jax.numpy as jnp
import numpy as np
from jax import lax
from jax.experimental import pallas as pl
from jax.experimental.pallas import tpu as pltpu
from jax.sharding import Mesh
from jax.sharding import PartitionSpec as P


AXES = ("xh", "core", "z", "y", "xl")
DP = ("xh", "core")
CENTRE = ("z", "y", "xl")

inverse_coolness_beta = 0.0625
LOG2E = float(np.log2(np.e))
LN2 = float(np.log(2.0))
CROSS2 = 2.0 * inverse_coolness_beta * LOG2E

LANES = 128
TILE = 256
CHUNKS = 4


def column_of(row):
    return jnp.transpose(jnp.broadcast_to(row, (LANES, LANES)))


def centre_bias(centres_ref, prior_ref):
    wide = centres_ref[...].astype(jnp.float32)
    norm = jnp.sum(wide * wide, axis=1, keepdims=True)
    prior = jnp.concatenate([column_of(prior_ref[k : k + 1, :]) for k in range(prior_ref.shape[0])])
    return (prior - norm * inverse_coolness_beta) * LOG2E


def cross_tile(centres_ref, rows):
    return lax.dot_general(
        centres_ref[...], rows, (((1,), (1,)), ((), ())), preferred_element_type=jnp.float32
    )


def stats_kernel(
    samples_hbm, centres_ref, prior_ref, out_ref, samples_ref, kept_ref, bias_ref, sems
):
    step = samples_ref.shape[0] // CHUNKS
    copies = []
    for k in range(CHUNKS):
        rows = pl.ds(k * step, step)
        copies.append(
            pltpu.make_async_copy(samples_hbm.at[rows, :], samples_ref.at[rows, :], sems.at[k])
        )
        copies[k].start()
    bias = centre_bias(centres_ref, prior_ref)
    bias_ref[...] = bias
    kept_ref[...] = centres_ref[...]
    for t in range(samples_ref.shape[0] // TILE):
        if t * TILE % step == 0:
            copies[t * TILE // step].wait()
        cross = cross_tile(centres_ref, samples_ref[t * TILE : (t + 1) * TILE, :])
        for h in range(TILE // LANES):
            score = cross[:, h * LANES : (h + 1) * LANES] * CROSS2 + bias
            top = jnp.max(score, axis=0, keepdims=True)
            total = jnp.sum(jnp.exp2(score - top), axis=0, keepdims=True)
            at = t * (TILE // LANES) + h
            out_ref[0, at : at + 1, :] = top + jnp.log2(total)
    for k in range(1, out_ref.shape[0]):
        out_ref[k, :, :] = out_ref[0, :, :]


def accumulate_kernel(samples_ref, centres_ref, bias_ref, parts_ref, out_ref, partition_ref):
    bias = bias_ref[...]
    partition_ref[...] = merged(parts_ref[...])
    local = centres_ref.shape[0]
    weighted = jnp.zeros((local, LANES), jnp.float32)
    mass = jnp.zeros((local, LANES), jnp.float32)
    for t in range(samples_ref.shape[0] // TILE):
        rows = samples_ref[t * TILE : (t + 1) * TILE, :]
        cross = cross_tile(centres_ref, rows)
        for h in range(TILE // LANES):
            at = t * (TILE // LANES) + h
            score = cross[:, h * LANES : (h + 1) * LANES] * CROSS2 + bias
            resp = jnp.exp2(score - partition_ref[at : at + 1, :]).astype(jnp.bfloat16)
            mass = mass + resp.astype(jnp.float32)
            weighted = weighted + lax.dot_general(
                resp,
                rows[h * LANES : (h + 1) * LANES, :],
                (((1,), (0,)), ((), ())),
                preferred_element_type=jnp.float32,
            )
    out_ref[0:local, :] = weighted
    out_ref[local:, :] = jnp.zeros((out_ref.shape[0] - local, LANES), jnp.float32)
    for k in range(local // LANES):
        block = jnp.transpose(mass[k * LANES : (k + 1) * LANES, :])
        out_ref[local + k : local + k + 1, :] = jnp.sum(block, axis=0, keepdims=True)


def finish_kernel(denominator, mine_ref, other_ref, centres_ref, new_ref, prior_ref):
    local = centres_ref.shape[0]
    for k in range(local // LANES):
        rows = slice(k * LANES, (k + 1) * LANES)
        at = slice(local + k, local + k + 1)
        mass = mine_ref[at, :] + other_ref[at, :] + 1.0
        prior_ref[k : k + 1, :] = jnp.log(mass / denominator)
        weighted = mine_ref[rows, :] + other_ref[rows, :]
        new_ref[rows, :] = (weighted + centres_ref[rows, :].astype(jnp.float32)) / column_of(mass)


def shared(copies, axes):
    return lax.all_to_all(copies, axes, 0, 0, tiled=True)


def on_chip(x):
    return pltpu.with_memory_space_constraint(x, pltpu.VMEM)


def merged(parts):
    top = jnp.max(parts, axis=0)
    return top + jnp.log2(jnp.sum(jnp.exp2(parts - top), axis=0))


def swapped(x, axis):
    return lax.ppermute(x, axis, [(0, 1), (1, 0)])


def shards(samples, centres, facility_prior_logprob):
    rows, features = samples.shape
    local = centres.shape[0]
    prior = facility_prior_logprob.reshape(local // LANES, LANES)
    lines = rows // LANES
    near, far = ("y", "xl"), "z"
    whole = pl.BlockSpec(memory_space=pltpu.VMEM)
    copies, samples_here, centres_here, bias = pl.pallas_call(
        stats_kernel,
        in_specs=[pl.BlockSpec(memory_space=pl.ANY), whole, whole],
        out_specs=[whole] * 4,
        out_shape=(
            pltpu.VMEM((lax.axis_size(near), lines, LANES), jnp.float32),
            pltpu.VMEM((rows, features), samples.dtype),
            pltpu.VMEM((local, features), centres.dtype),
            pltpu.VMEM((local, LANES), jnp.float32),
        ),
        scratch_shapes=[pltpu.SemaphoreType.DMA((CHUNKS,))],
    )(samples, centres, prior)
    part = merged(shared(copies, near))
    parts = shared(jnp.broadcast_to(part, (lax.axis_size(far), *part.shape)), far)
    sums, partition = pl.pallas_call(
        accumulate_kernel,
        in_specs=[whole, whole, whole, whole],
        out_specs=[whole, whole],
        out_shape=(
            pltpu.VMEM((local + 8, features), jnp.float32),
            pltpu.VMEM((lines, LANES), jnp.float32),
        ),
    )(on_chip(samples_here), on_chip(centres_here), on_chip(bias), on_chip(parts))
    sums = sums + swapped(sums, "core")
    other = swapped(sums, "xh")
    wide = samples_here.astype(jnp.float32)
    norms = jnp.sum(wide * wide, axis=1)
    log_partition = partition.reshape(rows) * LN2 - norms * inverse_coolness_beta
    denominator = float(rows * lax.axis_size(DP) + local * lax.axis_size(CENTRE))
    new_centres, new_log_prior = pl.pallas_call(
        lambda *refs: finish_kernel(denominator, *refs),
        in_specs=[whole, whole, whole],
        out_shape=(
            jax.ShapeDtypeStruct((local, features), jnp.float32),
            jax.ShapeDtypeStruct((local // LANES, LANES), jnp.float32),
        ),
    )(on_chip(sums), on_chip(other), on_chip(centres_here))
    return new_centres, new_log_prior.reshape(local), log_partition


def solution(mesh):
    torus = Mesh(mesh.devices.reshape(2, 2, 8, 4, 2), AXES)
    in_specs = (P(DP, None), P(CENTRE, None), P(CENTRE))
    out_specs = (P(CENTRE, None), P(CENTRE), P(DP))
    return jax.shard_map(
        shards, mesh=torus, in_specs=in_specs, out_specs=out_specs, check_vma=False
    )
```

```python
import jax
import jax.numpy as jnp
import numpy as np
from jax import lax
from jax.experimental import pallas as pl
from jax.experimental.pallas import tpu as pltpu
from jax.sharding import Mesh
from jax.sharding import PartitionSpec as P


AXES = ("xh", "core", "z", "y", "xl")
DP = ("xh", "core")
CENTRE = ("z", "y", "xl")

inverse_coolness_beta = 0.0625
LOG2E = float(np.log2(np.e))
LN2 = float(np.log(2.0))
CROSS2 = 2.0 * inverse_coolness_beta * LOG2E

LANES = 128
TILE = 256
CHUNKS = 2
SMALL = pltpu.CompilerParams(vmem_limit_bytes=16 << 20)


def column_of(row):
    return jnp.transpose(jnp.broadcast_to(row, (LANES, LANES)))


def centre_bias(centres_ref, prior_ref):
    wide = centres_ref[...].astype(jnp.float32)
    norm = jnp.sum(wide * wide, axis=1, keepdims=True)
    prior = jnp.concatenate([column_of(prior_ref[k : k + 1, :]) for k in range(prior_ref.shape[0])])
    return (prior - norm * inverse_coolness_beta) * LOG2E


def stats_kernel(
    samples_hbm, centres_hbm, prior_hbm, out_ref, samples_ref, centres_ref, scaled_ref, top_ref, prior_ref, sems
):
    pairs = [(centres_hbm, centres_ref), (prior_hbm, prior_ref)]
    step = samples_ref.shape[0] // CHUNKS
    for k in range(CHUNKS):
        rows = pl.ds(k * step, step)
        pairs.append((samples_hbm.at[rows, :], samples_ref.at[rows, :]))
    copies = [pltpu.make_async_copy(a, b, sems.at[k]) for k, (a, b) in enumerate(pairs)]
    for copy in copies:
        copy.start()
    copies[0].wait()
    copies[1].wait()
    bias = centre_bias(centres_ref, prior_ref)
    for t in range(samples_ref.shape[0] // TILE):
        if t * TILE % step == 0:
            copies[2 + t * TILE // step].wait()
        cross = lax.dot_general(
            centres_ref[...],
            samples_ref[t * TILE : (t + 1) * TILE, :],
            (((1,), (1,)), ((), ())),
            preferred_element_type=jnp.float32,
        )
        for h in range(TILE // LANES):
            at = t * (TILE // LANES) + h
            score = cross[:, h * LANES : (h + 1) * LANES] * CROSS2 + bias
            top = jnp.max(score, axis=0, keepdims=True)
            scaled = jnp.exp2(score - top)
            scaled_ref[:, at * LANES : (at + 1) * LANES] = scaled
            total = jnp.sum(scaled, axis=0, keepdims=True)
            top_ref[at : at + 1, :] = top
            out_ref[0, at : at + 1, :] = top + jnp.log2(total)
    for k in range(1, out_ref.shape[0]):
        out_ref[k, :, :] = out_ref[0, :, :]


def merge_kernel(parts_ref, out_ref):
    part = merged(parts_ref[...])
    for k in range(out_ref.shape[0]):
        out_ref[k, :, :] = part


def accumulate_kernel(samples_ref, scaled_ref, top_ref, parts_ref, out_ref, partition_ref, factor_ref):
    partition = merged(parts_ref[...])
    partition_ref[...] = partition
    factor_ref[...] = jnp.exp2(top_ref[...] - partition)
    local = scaled_ref.shape[0]
    sums = jnp.zeros((local, 2 * LANES), jnp.float32)
    ones = jnp.ones((TILE, LANES), jnp.bfloat16)
    for t in range(samples_ref.shape[0] // TILE):
        resp = []
        for h in range(TILE // LANES):
            at = t * (TILE // LANES) + h
            scaled = scaled_ref[:, at * LANES : (at + 1) * LANES]
            resp.append((scaled * factor_ref[at : at + 1, :]).astype(jnp.bfloat16))
        rows = samples_ref[t * TILE : (t + 1) * TILE, :]
        sums = sums + lax.dot_general(
            jnp.concatenate(resp, axis=1),
            jnp.concatenate([rows, ones], axis=1),
            (((1,), (0,)), ((), ())),
            preferred_element_type=jnp.float32,
        )
    out_ref[0:local, :] = sums[:, :LANES]
    out_ref[local:, :] = jnp.zeros((out_ref.shape[0] - local, LANES), jnp.float32)
    for k in range(local // LANES):
        block = jnp.transpose(sums[k * LANES : (k + 1) * LANES, LANES:])
        out_ref[local + k : local + k + 1, :] = block[0:1, :]


def finish_kernel(denominator, mine_ref, other_ref, centres_ref, new_ref, prior_ref):
    local = centres_ref.shape[0]
    for k in range(local // LANES):
        rows = slice(k * LANES, (k + 1) * LANES)
        at = slice(local + k, local + k + 1)
        mass = mine_ref[at, :] + other_ref[at, :] + 1.0
        prior_ref[k : k + 1, :] = jnp.log(mass / denominator)
        weighted = mine_ref[rows, :] + other_ref[rows, :]
        new_ref[rows, :] = (weighted + centres_ref[rows, :].astype(jnp.float32)) / column_of(mass)


def shared(copies, axes):
    return lax.all_to_all(copies, axes, 0, 0, tiled=True)


def on_chip(x):
    return pltpu.with_memory_space_constraint(x, pltpu.VMEM)


def merged(parts):
    top = jnp.max(parts, axis=0)
    return top + jnp.log2(jnp.sum(jnp.exp2(parts - top), axis=0))


def swapped(x, axis):
    return lax.ppermute(x, axis, [(0, 1), (1, 0)])


def shards(samples, centres, facility_prior_logprob):
    rows, features = samples.shape
    local = centres.shape[0]
    prior = facility_prior_logprob.reshape(local // LANES, LANES)
    lines = rows // LANES
    near, far = ("y", "xl"), "z"
    whole = pl.BlockSpec(memory_space=pltpu.VMEM)
    anywhere = pl.BlockSpec(memory_space=pl.ANY)
    copies, samples_here, centres_here, scaled, top = pl.pallas_call(
        stats_kernel,
        in_specs=[anywhere] * 3,
        out_specs=[whole] * 5,
        out_shape=(
            pltpu.VMEM((lax.axis_size(near), lines, LANES), jnp.float32),
            pltpu.VMEM((rows, features), samples.dtype),
            pltpu.VMEM((local, features), centres.dtype),
            pltpu.VMEM((local, rows), jnp.float32),
            pltpu.VMEM((lines, LANES), jnp.float32),
        ),
        compiler_params=SMALL,
        scratch_shapes=[
            pltpu.VMEM(prior.shape, jnp.float32),
            pltpu.SemaphoreType.DMA((CHUNKS + 2,)),
        ],
    )(samples, centres, prior)
    copies = pl.pallas_call(
        merge_kernel,
        in_specs=[whole],
        out_specs=whole,
        out_shape=pltpu.VMEM((lax.axis_size(far), lines, LANES), jnp.float32),
        compiler_params=SMALL,
    )(on_chip(shared(copies, near)))
    parts = shared(copies, far)
    sums, partition = pl.pallas_call(
        accumulate_kernel,
        in_specs=[whole] * 4,
        out_specs=[whole, whole],
        out_shape=(
            pltpu.VMEM((local + 8, features), jnp.float32),
            pltpu.VMEM((lines, LANES), jnp.float32),
        ),
        compiler_params=SMALL,
        scratch_shapes=[pltpu.VMEM((lines, LANES), jnp.float32)],
    )(on_chip(samples_here), on_chip(scaled), on_chip(top), on_chip(parts))
    other = swapped(sums, "xh")
    wide = samples_here.astype(jnp.float32)
    norms = jnp.sum(wide * wide, axis=1)
    log_partition = partition.reshape(rows) * LN2 - norms * inverse_coolness_beta
    sums = sums + other
    other = swapped(sums, "core")
    denominator = float(rows * lax.axis_size(DP) + local * lax.axis_size(CENTRE))
    new_centres, new_log_prior = pl.pallas_call(
        lambda *refs: finish_kernel(denominator, *refs),
        in_specs=[whole, whole, whole],
        out_shape=(
            jax.ShapeDtypeStruct((local, features), jnp.float32),
            jax.ShapeDtypeStruct((local // LANES, LANES), jnp.float32),
        ),
    )(on_chip(sums), on_chip(other), on_chip(centres_here))
    return new_centres, new_log_prior.reshape(local), log_partition


def solution(mesh):
    torus = Mesh(mesh.devices.reshape(2, 2, 8, 4, 2), AXES)
    in_specs = (P(DP, None), P(CENTRE, None), P(CENTRE))
    out_specs = (P(CENTRE, None), P(CENTRE), P(DP))
    return jax.shard_map(
        shards, mesh=torus, in_specs=in_specs, out_specs=out_specs, check_vma=False
    )
```

```python
import jax
import jax.numpy as jnp
import numpy as np
from jax import lax
from jax.experimental import pallas as pl
from jax.experimental.pallas import tpu as pltpu
from jax.sharding import Mesh
from jax.sharding import PartitionSpec as P


AXES = ("xh", "core", "z", "y", "xl")
DP = ("xh", "core")
CENTRE = ("z", "y", "xl")

inverse_coolness_beta = 0.0625
LOG2E = float(np.log2(np.e))
LN2 = float(np.log(2.0))
CROSS2 = 2.0 * inverse_coolness_beta * LOG2E

LANES = 128
TILE = 256
CHUNKS = 4
SMALL = pltpu.CompilerParams(vmem_limit_bytes=16 << 20)


def column_of(row):
    return jnp.transpose(jnp.broadcast_to(row, (LANES, LANES)))


def bias_parts(centres_ref, prior_ref):
    wide = centres_ref[...].astype(jnp.float32)
    norm = jnp.sum(wide * wide, axis=1, keepdims=True)
    prior = jnp.concatenate([column_of(prior_ref[k : k + 1, :]) for k in range(prior_ref.shape[0])])
    rest = prior * (0.5 / inverse_coolness_beta) - norm * 0.5
    lane = lax.broadcasted_iota(jnp.int32, rest.shape, 1)
    parts = jnp.zeros(rest.shape, jnp.float32)
    for k in range(3):
        part = rest.astype(jnp.bfloat16).astype(jnp.float32)
        parts = jnp.where(lane == k, part, parts)
        rest = rest - part
    return parts.astype(jnp.bfloat16)


def stats_kernel(
    samples_hbm, centres_hbm, prior_hbm, out_ref, samples_ref, centres_ref, scaled_ref, top_ref, prior_ref, sems
):
    pairs = [(centres_hbm, centres_ref), (prior_hbm, prior_ref)]
    step = samples_ref.shape[0] // CHUNKS
    for k in range(CHUNKS):
        rows = pl.ds(k * step, step)
        pairs.append((samples_hbm.at[rows, :], samples_ref.at[rows, :]))
    copies = [pltpu.make_async_copy(a, b, sems.at[k]) for k, (a, b) in enumerate(pairs)]
    for copy in copies:
        copy.start()
    copies[0].wait()
    copies[1].wait()
    extended = jnp.concatenate([centres_ref[...], bias_parts(centres_ref, prior_ref)], axis=1)
    ones = jnp.ones((TILE, LANES), jnp.bfloat16)

    def scores(t):
        rows = samples_ref[pl.ds(t * TILE, TILE), :]
        return lax.dot_general(
            extended,
            jnp.concatenate([rows, ones], axis=1),
            (((1,), (1,)), ((), ())),
            preferred_element_type=jnp.float32,
        )

    def reduce(t, score):
        for h in range(TILE // LANES):
            at = t * (TILE // LANES) + h
            half = score[:, h * LANES : (h + 1) * LANES]
            top = jnp.max(half, axis=0, keepdims=True)
            scaled = jnp.exp2((half - top) * CROSS2)
            scaled_ref[at, :, :] = scaled
            total = jnp.sum(scaled, axis=0, keepdims=True)
            top_ref[pl.ds(at, 1), :] = top * CROSS2
            out_ref[0, pl.ds(at, 1), :] = top * CROSS2 + jnp.log2(total)

    for copy in copies[2:]:
        copy.wait()
    tiles = samples_ref.shape[0] // TILE
    ahead = scores(0)
    for t in range(tiles):
        score, ahead = ahead, scores(min(t + 1, tiles - 1))
        reduce(t, score)
    for k in range(1, out_ref.shape[0]):
        out_ref[k, :, :] = out_ref[0, :, :]


def merge_kernel(parts_ref, out_ref):
    part = merged(parts_ref[...])
    for k in range(out_ref.shape[0]):
        out_ref[k, :, :] = part


def accumulate_kernel(samples_ref, scaled_ref, top_ref, parts_ref, out_ref, partition_ref, factor_ref):
    partition = merged(parts_ref[...])
    partition_ref[...] = partition
    factor_ref[...] = jnp.exp2(top_ref[...] - partition)
    local = scaled_ref.shape[1]
    sums = jnp.zeros((local, 2 * LANES), jnp.float32)
    ones = jnp.ones((TILE, LANES), jnp.bfloat16)
    for t in range(samples_ref.shape[0] // TILE):
        resp = []
        for h in range(TILE // LANES):
            at = t * (TILE // LANES) + h
            scaled = scaled_ref[at]
            resp.append((scaled * factor_ref[at : at + 1, :]).astype(jnp.bfloat16))
        rows = samples_ref[t * TILE : (t + 1) * TILE, :]
        sums = sums + lax.dot_general(
            jnp.concatenate(resp, axis=1),
            jnp.concatenate([rows, ones], axis=1),
            (((1,), (0,)), ((), ())),
            preferred_element_type=jnp.float32,
        )
    out_ref[0:local, :] = sums[:, :LANES]
    out_ref[local:, :] = jnp.zeros((out_ref.shape[0] - local, LANES), jnp.float32)
    for k in range(local // LANES):
        block = jnp.transpose(sums[k * LANES : (k + 1) * LANES, LANES:])
        out_ref[local + k : local + k + 1, :] = block[0:1, :]


def finish_kernel(denominator, mine_ref, other_ref, centres_ref, new_ref, prior_ref):
    local = centres_ref.shape[0]
    for k in range(local // LANES):
        rows = slice(k * LANES, (k + 1) * LANES)
        at = slice(local + k, local + k + 1)
        mass = mine_ref[at, :] + other_ref[at, :] + 1.0
        prior_ref[k : k + 1, :] = jnp.log(mass / denominator)
        weighted = mine_ref[rows, :] + other_ref[rows, :]
        new_ref[rows, :] = (weighted + centres_ref[rows, :].astype(jnp.float32)) / column_of(mass)


def shared(copies, axes):
    return lax.all_to_all(copies, axes, 0, 0, tiled=True)


def on_chip(x):
    return pltpu.with_memory_space_constraint(x, pltpu.VMEM)


def in_hbm(x):
    return pltpu.with_memory_space_constraint(x, pltpu.HBM)


def merged(parts):
    top = jnp.max(parts, axis=0)
    return top + jnp.log2(jnp.sum(jnp.exp2(parts - top), axis=0))


def swapped(x, axis):
    return lax.ppermute(x, axis, [(0, 1), (1, 0)])


def shards(samples, centres, facility_prior_logprob):
    rows, features = samples.shape
    local = centres.shape[0]
    prior = facility_prior_logprob.reshape(local // LANES, LANES)
    lines = rows // LANES
    near, far = ("y", "xl"), "z"
    whole = pl.BlockSpec(memory_space=pltpu.VMEM)
    copies, samples_here, centres_here, scaled, top = pl.pallas_call(
        stats_kernel,
        in_specs=[pl.BlockSpec(memory_space=pltpu.HBM)] * 3,
        out_specs=[whole] * 5,
        out_shape=(
            pltpu.VMEM((lax.axis_size(near), lines, LANES), jnp.float32),
            pltpu.VMEM((rows, features), samples.dtype),
            pltpu.VMEM((local, features), centres.dtype),
            pltpu.VMEM((lines, local, LANES), jnp.float32),
            pltpu.VMEM((lines, LANES), jnp.float32),
        ),
        compiler_params=SMALL,
        scratch_shapes=[
            pltpu.VMEM(prior.shape, jnp.float32),
            pltpu.SemaphoreType.DMA((CHUNKS + 2,)),
        ],
    )(in_hbm(samples), in_hbm(centres), in_hbm(prior))
    copies = pl.pallas_call(
        merge_kernel,
        in_specs=[whole],
        out_specs=whole,
        out_shape=pltpu.VMEM((lax.axis_size(far), lines, LANES), jnp.float32),
        compiler_params=SMALL,
    )(on_chip(shared(copies, near)))
    parts = shared(copies, far)
    sums, partition = pl.pallas_call(
        accumulate_kernel,
        in_specs=[whole] * 4,
        out_specs=[whole, whole],
        out_shape=(
            pltpu.VMEM((local + 8, features), jnp.float32),
            pltpu.VMEM((lines, LANES), jnp.float32),
        ),
        compiler_params=SMALL,
        scratch_shapes=[pltpu.VMEM((lines, LANES), jnp.float32)],
    )(on_chip(samples_here), on_chip(scaled), on_chip(top), on_chip(parts))
    other = swapped(sums, "xh")
    wide = samples_here.astype(jnp.float32)
    norms = jnp.sum(wide * wide, axis=1)
    log_partition = partition.reshape(rows) * LN2 - norms * inverse_coolness_beta
    sums = sums + other
    other = swapped(sums, "core")
    denominator = float(rows * lax.axis_size(DP) + local * lax.axis_size(CENTRE))
    new_centres, new_log_prior = pl.pallas_call(
        lambda *refs: finish_kernel(denominator, *refs),
        in_specs=[whole, whole, whole],
        out_shape=(
            jax.ShapeDtypeStruct((local, features), jnp.float32),
            jax.ShapeDtypeStruct((local // LANES, LANES), jnp.float32),
        ),
    )(on_chip(sums), on_chip(other), on_chip(centres_here))
    return new_centres, new_log_prior.reshape(local), log_partition


def solution(mesh):
    torus = Mesh(mesh.devices.reshape(2, 2, 8, 4, 2), AXES)
    in_specs = (P(DP, None), P(CENTRE, None), P(CENTRE))
    out_specs = (P(CENTRE, None), P(CENTRE), P(DP))
    return jax.shard_map(
        shards, mesh=torus, in_specs=in_specs, out_specs=out_specs, check_vma=False
    )
```

```python
import jax
import jax.numpy as jnp
import numpy as np
from jax import lax
from jax.experimental import pallas as pl
from jax.experimental.pallas import tpu as pltpu
from jax.sharding import Mesh
from jax.sharding import PartitionSpec as P


AXES = ("xh", "core", "z", "yx")
DP = ("xh", "core")
CENTRE = ("z", "yx")
MEMBERS = {"z": [4, 3, 2, 1, 5, 6, 7, 0], "yx": [5, 7, 6, 1, 4, 3, 2, 0]}

inverse_coolness_beta = 0.0625
LOG2E = float(np.log2(np.e))
LN2 = float(np.log(2.0))
CROSS2 = 2.0 * inverse_coolness_beta * LOG2E

LANES = 128
TILE = 256
CHUNKS = 4
SMALL = pltpu.CompilerParams(vmem_limit_bytes=16 << 20)


def column_of(row):
    return jnp.transpose(jnp.broadcast_to(row, (LANES, LANES)))


def bias_parts(centres_ref, prior_ref):
    wide = centres_ref[...].astype(jnp.float32)
    norm = jnp.sum(wide * wide, axis=1, keepdims=True)
    prior = jnp.concatenate([column_of(prior_ref[k : k + 1, :]) for k in range(prior_ref.shape[0])])
    rest = prior * (0.5 / inverse_coolness_beta) - norm * 0.5
    lane = lax.broadcasted_iota(jnp.int32, rest.shape, 1)
    parts = jnp.zeros(rest.shape, jnp.float32)
    for k in range(3):
        part = rest.astype(jnp.bfloat16).astype(jnp.float32)
        parts = jnp.where(lane == k, part, parts)
        rest = rest - part
    return parts.astype(jnp.bfloat16)


def stats_kernel(
    samples_hbm, centres_hbm, prior_hbm, out_ref, samples_ref, centres_ref, scaled_ref, top_ref, prior_ref, sems
):
    pairs = [(centres_hbm, centres_ref), (prior_hbm, prior_ref)]
    step = samples_ref.shape[0] // CHUNKS
    for k in range(CHUNKS):
        rows = pl.ds(k * step, step)
        pairs.append((samples_hbm.at[rows, :], samples_ref.at[rows, :]))
    copies = [pltpu.make_async_copy(a, b, sems.at[k]) for k, (a, b) in enumerate(pairs)]
    for copy in copies:
        copy.start()
    copies[0].wait()
    copies[1].wait()
    extended = jnp.concatenate([centres_ref[...], bias_parts(centres_ref, prior_ref)], axis=1)
    ones = jnp.ones((TILE, LANES), jnp.bfloat16)

    def scores(t):
        rows = samples_ref[pl.ds(t * TILE, TILE), :]
        return lax.dot_general(
            extended,
            jnp.concatenate([rows, ones], axis=1),
            (((1,), (1,)), ((), ())),
            preferred_element_type=jnp.float32,
        )

    def reduce(t, score):
        for h in range(TILE // LANES):
            at = t * (TILE // LANES) + h
            half = score[:, h * LANES : (h + 1) * LANES]
            top = jnp.max(half, axis=0, keepdims=True)
            scaled = jnp.exp2((half - top) * CROSS2)
            scaled_ref[at, :, :] = scaled
            total = jnp.sum(scaled, axis=0, keepdims=True)
            top_ref[pl.ds(at, 1), :] = top * CROSS2
            out_ref[0, pl.ds(at, 1), :] = top * CROSS2 + jnp.log2(total)

    for copy in copies[2:]:
        copy.wait()
    tiles = samples_ref.shape[0] // TILE
    ahead = scores(0)
    for t in range(tiles):
        score, ahead = ahead, scores(min(t + 1, tiles - 1))
        reduce(t, score)
    for k in range(1, out_ref.shape[0]):
        out_ref[k, :, :] = out_ref[0, :, :]


def merge_kernel(parts_ref, out_ref):
    part = merged(parts_ref[...])
    for k in range(out_ref.shape[0]):
        out_ref[k, :, :] = part


def accumulate_kernel(samples_ref, scaled_ref, top_ref, parts_ref, out_ref, partition_ref, factor_ref):
    partition = merged(parts_ref[...])
    partition_ref[...] = partition
    factor_ref[...] = jnp.exp2(top_ref[...] - partition)
    local = scaled_ref.shape[1]
    sums = jnp.zeros((local, 2 * LANES), jnp.float32)
    ones = jnp.ones((TILE, LANES), jnp.bfloat16)
    for t in range(samples_ref.shape[0] // TILE):
        resp = []
        for h in range(TILE // LANES):
            at = t * (TILE // LANES) + h
            scaled = scaled_ref[at]
            resp.append((scaled * factor_ref[at : at + 1, :]).astype(jnp.bfloat16))
        rows = samples_ref[t * TILE : (t + 1) * TILE, :]
        sums = sums + lax.dot_general(
            jnp.concatenate(resp, axis=1),
            jnp.concatenate([rows, ones], axis=1),
            (((1,), (0,)), ((), ())),
            preferred_element_type=jnp.float32,
        )
    out_ref[0:local, :] = sums[:, :LANES]
    out_ref[local:, :] = jnp.zeros((out_ref.shape[0] - local, LANES), jnp.float32)
    for k in range(local // LANES):
        block = jnp.transpose(sums[k * LANES : (k + 1) * LANES, LANES:])
        out_ref[local + k : local + k + 1, :] = block[0:1, :]


def finish_kernel(denominator, mine_ref, other_ref, centres_ref, new_ref, prior_ref):
    local = centres_ref.shape[0]
    for k in range(local // LANES):
        rows = slice(k * LANES, (k + 1) * LANES)
        at = slice(local + k, local + k + 1)
        mass = mine_ref[at, :] + other_ref[at, :] + 1.0
        prior_ref[k : k + 1, :] = jnp.log(mass / denominator)
        weighted = mine_ref[rows, :] + other_ref[rows, :]
        new_ref[rows, :] = (weighted + centres_ref[rows, :].astype(jnp.float32)) / column_of(mass)


def shared(copies, axis):
    return lax.all_to_all(copies, axis, 0, 0, axis_index_groups=[MEMBERS[axis]], tiled=True)


def on_chip(x):
    return pltpu.with_memory_space_constraint(x, pltpu.VMEM)


def in_hbm(x):
    return pltpu.with_memory_space_constraint(x, pltpu.HBM)


def merged(parts):
    top = jnp.max(parts, axis=0)
    return top + jnp.log2(jnp.sum(jnp.exp2(parts - top), axis=0))


def swapped(x, axis):
    return lax.ppermute(x, axis, [(0, 1), (1, 0)])


def shards(samples, centres, facility_prior_logprob):
    rows, features = samples.shape
    local = centres.shape[0]
    prior = facility_prior_logprob.reshape(local // LANES, LANES)
    lines = rows // LANES
    near, far = "yx", "z"
    whole = pl.BlockSpec(memory_space=pltpu.VMEM)
    copies, samples_here, centres_here, scaled, top = pl.pallas_call(
        stats_kernel,
        in_specs=[pl.BlockSpec(memory_space=pltpu.HBM)] * 3,
        out_specs=[whole] * 5,
        out_shape=(
            pltpu.VMEM((lax.axis_size(near), lines, LANES), jnp.float32),
            pltpu.VMEM((rows, features), samples.dtype),
            pltpu.VMEM((local, features), centres.dtype),
            pltpu.VMEM((lines, local, LANES), jnp.float32),
            pltpu.VMEM((lines, LANES), jnp.float32),
        ),
        compiler_params=SMALL,
        scratch_shapes=[
            pltpu.VMEM(prior.shape, jnp.float32),
            pltpu.SemaphoreType.DMA((CHUNKS + 2,)),
        ],
    )(in_hbm(samples), in_hbm(centres), in_hbm(prior))
    copies = pl.pallas_call(
        merge_kernel,
        in_specs=[whole],
        out_specs=whole,
        out_shape=pltpu.VMEM((lax.axis_size(far), lines, LANES), jnp.float32),
        compiler_params=SMALL,
    )(on_chip(shared(copies, near)))
    parts = shared(copies, far)
    sums, partition = pl.pallas_call(
        accumulate_kernel,
        in_specs=[whole] * 4,
        out_specs=[whole, whole],
        out_shape=(
            pltpu.VMEM((local + 8, features), jnp.float32),
            pltpu.VMEM((lines, LANES), jnp.float32),
        ),
        compiler_params=SMALL,
        scratch_shapes=[pltpu.VMEM((lines, LANES), jnp.float32)],
    )(on_chip(samples_here), on_chip(scaled), on_chip(top), on_chip(parts))
    other = swapped(sums, "xh")
    wide = samples_here.astype(jnp.float32)
    norms = jnp.sum(wide * wide, axis=1)
    log_partition = partition.reshape(rows) * LN2 - norms * inverse_coolness_beta
    sums = sums + other
    other = swapped(sums, "core")
    denominator = float(rows * lax.axis_size(DP) + local * lax.axis_size(CENTRE))
    new_centres, new_log_prior = pl.pallas_call(
        lambda *refs: finish_kernel(denominator, *refs),
        in_specs=[whole, whole, whole],
        out_shape=(
            jax.ShapeDtypeStruct((local, features), jnp.float32),
            jax.ShapeDtypeStruct((local // LANES, LANES), jnp.float32),
        ),
    )(on_chip(sums), on_chip(other), on_chip(centres_here))
    return new_centres, new_log_prior.reshape(local), log_partition


def solution(mesh):
    torus = Mesh(mesh.devices.reshape(2, 2, 8, 8), AXES)
    in_specs = (P(DP, None), P(CENTRE, None), P(CENTRE))
    out_specs = (P(CENTRE, None), P(CENTRE), P(DP))
    return jax.shard_map(
        shards, mesh=torus, in_specs=in_specs, out_specs=out_specs, check_vma=False
    )
```

```python
import jax
import jax.numpy as jnp
import numpy as np
from jax import lax
from jax.experimental import pallas as pl
from jax.experimental.pallas import tpu as pltpu
from jax.sharding import Mesh
from jax.sharding import PartitionSpec as P


AXES = ("xh", "core", "z", "yx")
DP = ("xh", "core")
CENTRE = ("z", "yx")
MEMBERS = {"z": [5, 4, 3, 2, 6, 7, 0, 1], "yx": [5, 7, 6, 1, 4, 3, 2, 0]}

inverse_coolness_beta = 0.0625
LOG2E = float(np.log2(np.e))
LN2 = float(np.log(2.0))
CROSS2 = 2.0 * inverse_coolness_beta * LOG2E

LANES = 128
TILE = 256
CHUNKS = 4
ACC = 4
SMALL = pltpu.CompilerParams(vmem_limit_bytes=16 << 20)


def column_of(row):
    return jnp.transpose(jnp.broadcast_to(row, (LANES, LANES)))


def bias_parts(centres_ref, prior_ref):
    wide = centres_ref[...].astype(jnp.float32)
    norm = jnp.sum(wide * wide, axis=1, keepdims=True)
    prior = jnp.concatenate([column_of(prior_ref[k : k + 1, :]) for k in range(prior_ref.shape[0])])
    rest = prior * (0.5 / inverse_coolness_beta) - norm * 0.5
    lane = lax.broadcasted_iota(jnp.int32, rest.shape, 1)
    parts = jnp.zeros(rest.shape, jnp.float32)
    for k in range(3):
        part = rest.astype(jnp.bfloat16).astype(jnp.float32)
        parts = jnp.where(lane == k, part, parts)
        rest = rest - part
    return parts.astype(jnp.bfloat16)


def stats_kernel(
    samples_hbm, centres_hbm, prior_hbm, out_ref, samples_ref, centres_ref, scaled_ref, top_ref, prior_ref, score_ref, sems
):
    pairs = [(centres_hbm, centres_ref), (prior_hbm, prior_ref)]
    step = samples_ref.shape[0] // CHUNKS
    for k in range(CHUNKS):
        rows = pl.ds(k * step, step)
        pairs.append((samples_hbm.at[rows, :], samples_ref.at[rows, :]))
    copies = [pltpu.make_async_copy(a, b, sems.at[k]) for k, (a, b) in enumerate(pairs)]
    for copy in copies:
        copy.start()
    copies[0].wait()
    copies[1].wait()
    extended = jnp.concatenate([centres_ref[...], bias_parts(centres_ref, prior_ref)], axis=1)
    ones = jnp.ones((TILE, LANES), jnp.bfloat16)

    def scores(t):
        rows = samples_ref[pl.ds(t * TILE, TILE), :]
        return lax.dot_general(
            extended,
            jnp.concatenate([rows, ones], axis=1),
            (((1,), (1,)), ((), ())),
            preferred_element_type=jnp.float32,
        )

    def reduce(t):
        slot = t % 2
        for h in range(TILE // LANES):
            at = t * (TILE // LANES) + h
            lanes = slice(h * LANES, (h + 1) * LANES)
            tops = [score_ref[slot, 8 * r : 8 * r + 8, lanes] for r in range(ACC)]
            for r in range(ACC, local // 8):
                tops[r % ACC] = jnp.maximum(tops[r % ACC], score_ref[slot, 8 * r : 8 * r + 8, lanes])
            while len(tops) > 1:
                tops = [jnp.maximum(a, c) for a, c in zip(tops[::2], tops[1::2])]
            top = jnp.max(tops[0], axis=0, keepdims=True)
            totals = [None] * ACC
            for r in range(local // 8):
                scaled = jnp.exp2((score_ref[slot, 8 * r : 8 * r + 8, lanes] - top) * CROSS2)
                scaled_ref[at, 8 * r : 8 * r + 8, :] = scaled
                totals[r % ACC] = scaled if totals[r % ACC] is None else totals[r % ACC] + scaled
            while len(totals) > 1:
                totals = [a + c for a, c in zip(totals[::2], totals[1::2])]
            total = jnp.sum(totals[0], axis=0, keepdims=True)
            top_ref[at : at + 1, :] = top * CROSS2
            out_ref[0, at : at + 1, :] = top * CROSS2 + jnp.log2(total)

    for copy in copies[2:]:
        copy.wait()
    tiles = samples_ref.shape[0] // TILE
    local = centres_ref.shape[0]
    score_ref[0, :, :] = scores(0)
    for t in range(tiles):
        if t + 1 < tiles:
            score_ref[(t + 1) % 2, :, :] = scores(t + 1)
        reduce(t)
    for k in range(1, out_ref.shape[0]):
        out_ref[k, :, :] = out_ref[0, :, :]


def merge_kernel(parts_ref, out_ref):
    part = merged(parts_ref[...])
    for k in range(out_ref.shape[0]):
        out_ref[k, :, :] = part


def accumulate_kernel(samples_ref, scaled_ref, top_ref, parts_ref, out_ref, partition_ref, factor_ref):
    partition = merged(parts_ref[...])
    partition_ref[...] = partition
    factor_ref[...] = jnp.exp2(top_ref[...] - partition)
    local = scaled_ref.shape[1]
    sums = jnp.zeros((local, 2 * LANES), jnp.float32)
    ones = jnp.ones((TILE, LANES), jnp.bfloat16)
    for t in range(samples_ref.shape[0] // TILE):
        resp = []
        for h in range(TILE // LANES):
            at = t * (TILE // LANES) + h
            scaled = scaled_ref[at]
            resp.append((scaled * factor_ref[at : at + 1, :]).astype(jnp.bfloat16))
        rows = samples_ref[t * TILE : (t + 1) * TILE, :]
        sums = sums + lax.dot_general(
            jnp.concatenate(resp, axis=1),
            jnp.concatenate([rows, ones], axis=1),
            (((1,), (0,)), ((), ())),
            preferred_element_type=jnp.float32,
        )
    out_ref[0:local, :] = sums[:, :LANES]
    out_ref[local:, :] = jnp.zeros((out_ref.shape[0] - local, LANES), jnp.float32)
    for k in range(local // LANES):
        block = jnp.transpose(sums[k * LANES : (k + 1) * LANES, LANES:])
        out_ref[local + k : local + k + 1, :] = block[0:1, :]


def finish_kernel(denominator, mine_ref, other_ref, centres_ref, new_ref, prior_ref):
    local = centres_ref.shape[0]
    for k in range(local // LANES):
        rows = slice(k * LANES, (k + 1) * LANES)
        at = slice(local + k, local + k + 1)
        mass = mine_ref[at, :] + other_ref[at, :] + 1.0
        prior_ref[k : k + 1, :] = jnp.log(mass / denominator)
        weighted = mine_ref[rows, :] + other_ref[rows, :]
        new_ref[rows, :] = (weighted + centres_ref[rows, :].astype(jnp.float32)) / column_of(mass)


def shared(copies, axis):
    return lax.all_to_all(copies, axis, 0, 0, axis_index_groups=[MEMBERS[axis]], tiled=True)


def on_chip(x):
    return pltpu.with_memory_space_constraint(x, pltpu.VMEM)


def in_hbm(x):
    return pltpu.with_memory_space_constraint(x, pltpu.HBM)


def merged(parts):
    top = jnp.max(parts, axis=0)
    return top + jnp.log2(jnp.sum(jnp.exp2(parts - top), axis=0))


def swapped(x, axis):
    return lax.ppermute(x, axis, [(0, 1), (1, 0)])


def shards(samples, centres, facility_prior_logprob):
    rows, features = samples.shape
    local = centres.shape[0]
    prior = facility_prior_logprob.reshape(local // LANES, LANES)
    lines = rows // LANES
    near, far = "yx", "z"
    whole = pl.BlockSpec(memory_space=pltpu.VMEM)
    copies, samples_here, centres_here, scaled, top = pl.pallas_call(
        stats_kernel,
        in_specs=[pl.BlockSpec(memory_space=pltpu.HBM)] * 3,
        out_specs=[whole] * 5,
        out_shape=(
            pltpu.VMEM((lax.axis_size(near), lines, LANES), jnp.float32),
            pltpu.VMEM((rows, features), samples.dtype),
            pltpu.VMEM((local, features), centres.dtype),
            pltpu.VMEM((lines, local, LANES), jnp.float32),
            pltpu.VMEM((lines, LANES), jnp.float32),
        ),
        compiler_params=SMALL,
        scratch_shapes=[
            pltpu.VMEM(prior.shape, jnp.float32),
            pltpu.VMEM((2, local, TILE), jnp.float32),
            pltpu.SemaphoreType.DMA((CHUNKS + 2,)),
        ],
    )(in_hbm(samples), in_hbm(centres), in_hbm(prior))
    copies = pl.pallas_call(
        merge_kernel,
        in_specs=[whole],
        out_specs=whole,
        out_shape=pltpu.VMEM((lax.axis_size(far), lines, LANES), jnp.float32),
        compiler_params=SMALL,
    )(on_chip(shared(copies, near)))
    parts = shared(copies, far)
    sums, partition = pl.pallas_call(
        accumulate_kernel,
        in_specs=[whole] * 4,
        out_specs=[whole, whole],
        out_shape=(
            pltpu.VMEM((local + 8, features), jnp.float32),
            pltpu.VMEM((lines, LANES), jnp.float32),
        ),
        compiler_params=SMALL,
        scratch_shapes=[pltpu.VMEM((lines, LANES), jnp.float32)],
    )(on_chip(samples_here), on_chip(scaled), on_chip(top), on_chip(parts))
    other = swapped(sums, "xh")
    wide = samples_here.astype(jnp.float32)
    norms = jnp.sum(wide * wide, axis=1)
    log_partition = partition.reshape(rows) * LN2 - norms * inverse_coolness_beta
    sums = sums + other
    other = swapped(sums, "core")
    denominator = float(rows * lax.axis_size(DP) + local * lax.axis_size(CENTRE))
    new_centres, new_log_prior = pl.pallas_call(
        lambda *refs: finish_kernel(denominator, *refs),
        in_specs=[whole, whole, whole],
        out_shape=(
            jax.ShapeDtypeStruct((local, features), jnp.float32),
            jax.ShapeDtypeStruct((local // LANES, LANES), jnp.float32),
        ),
    )(on_chip(sums), on_chip(other), on_chip(centres_here))
    return new_centres, new_log_prior.reshape(local), log_partition


def solution(mesh):
    torus = Mesh(mesh.devices.reshape(2, 2, 8, 8), AXES)
    in_specs = (P(DP, None), P(CENTRE, None), P(CENTRE))
    out_specs = (P(CENTRE, None), P(CENTRE), P(DP))
    return jax.shard_map(
        shards, mesh=torus, in_specs=in_specs, out_specs=out_specs, check_vma=False
    )
```

```python
import jax
import jax.numpy as jnp
import numpy as np
from jax import lax
from jax.experimental import pallas as pl
from jax.experimental.pallas import tpu as pltpu
from jax.sharding import Mesh
from jax.sharding import PartitionSpec as P


AXES = ("xh", "core", "z", "yx")
DP = ("xh", "core")
CENTRE = ("z", "yx")
MEMBERS = {"z": [5, 4, 3, 2, 6, 7, 0, 1], "yx": [5, 1, 7, 3, 4, 0, 6, 2]}

inverse_coolness_beta = 0.0625
LOG2E = float(np.log2(np.e))
LN2 = float(np.log(2.0))
CROSS2 = 2.0 * inverse_coolness_beta * LOG2E

LANES = 128
TILE = 256
CHUNKS = 4
ACC = 4
SMALL = pltpu.CompilerParams(vmem_limit_bytes=16 << 20)


def column_of(row):
    return jnp.transpose(jnp.broadcast_to(row, (LANES, LANES)))


def bias_parts(centres_ref, prior_ref):
    wide = centres_ref[...].astype(jnp.float32)
    norm = jnp.sum(wide * wide, axis=1, keepdims=True)
    prior = jnp.concatenate([column_of(prior_ref[k : k + 1, :]) for k in range(prior_ref.shape[0])])
    rest = prior * (0.5 / inverse_coolness_beta) - norm * 0.5
    lane = lax.broadcasted_iota(jnp.int32, rest.shape, 1)
    parts = jnp.zeros(rest.shape, jnp.float32)
    for k in range(3):
        part = rest.astype(jnp.bfloat16).astype(jnp.float32)
        parts = jnp.where(lane == k, part, parts)
        rest = rest - part
    return parts.astype(jnp.bfloat16)


def stats_kernel(
    samples_hbm, centres_hbm, prior_hbm, out_ref, samples_ref, centres_ref, scaled_ref, top_ref, prior_ref, score_ref, sems
):
    pairs = [(centres_hbm, centres_ref), (prior_hbm, prior_ref)]
    step = samples_ref.shape[0] // CHUNKS
    for k in range(CHUNKS):
        rows = pl.ds(k * step, step)
        pairs.append((samples_hbm.at[rows, :], samples_ref.at[rows, :]))
    copies = [pltpu.make_async_copy(a, b, sems.at[k]) for k, (a, b) in enumerate(pairs)]
    for copy in copies:
        copy.start()
    copies[0].wait()
    copies[1].wait()
    extended = jnp.concatenate([centres_ref[...], bias_parts(centres_ref, prior_ref)], axis=1)
    ones = jnp.ones((TILE, LANES), jnp.bfloat16)

    def scores(at):
        rows = samples_ref[at, :]
        return lax.dot_general(
            extended,
            jnp.concatenate([rows, ones[: rows.shape[0], :]], axis=1),
            (((1,), (1,)), ((), ())),
            preferred_element_type=jnp.float32,
        )

    def reduce(t):
        slot = t % 2
        for h in range(TILE // LANES):
            at = t * (TILE // LANES) + h
            lanes = slice(h * LANES, (h + 1) * LANES)
            tops = [score_ref[slot, 8 * r : 8 * r + 8, lanes] for r in range(ACC)]
            for r in range(ACC, local // 8):
                tops[r % ACC] = jnp.maximum(tops[r % ACC], score_ref[slot, 8 * r : 8 * r + 8, lanes])
            while len(tops) > 1:
                tops = [jnp.maximum(a, c) for a, c in zip(tops[::2], tops[1::2])]
            top = jnp.max(tops[0], axis=0, keepdims=True)
            totals = [None] * ACC
            for r in range(local // 8):
                scaled = jnp.exp2((score_ref[slot, 8 * r : 8 * r + 8, lanes] - top) * CROSS2)
                scaled_ref[at, 8 * r : 8 * r + 8, :] = scaled
                totals[r % ACC] = scaled if totals[r % ACC] is None else totals[r % ACC] + scaled
            while len(totals) > 1:
                totals = [a + c for a, c in zip(totals[::2], totals[1::2])]
            total = jnp.sum(totals[0], axis=0, keepdims=True)
            top_ref[at : at + 1, :] = top * CROSS2
            out_ref[0, at : at + 1, :] = top * CROSS2 + jnp.log2(total)

    for copy in copies[2:]:
        copy.wait()
    tiles = samples_ref.shape[0] // TILE
    local = centres_ref.shape[0]
    for h in range(TILE // LANES):
        lanes = slice(h * LANES, (h + 1) * LANES)
        score_ref[0, :, lanes] = scores(lanes)
    for t in range(tiles):
        if t + 1 < tiles:
            score_ref[(t + 1) % 2, :, :] = scores(slice((t + 1) * TILE, (t + 2) * TILE))
        reduce(t)
    for k in range(1, out_ref.shape[0]):
        out_ref[k, :, :] = out_ref[0, :, :]


def merge_kernel(parts_ref, out_ref):
    part = merged(parts_ref[...])
    for k in range(out_ref.shape[0]):
        out_ref[k, :, :] = part


def accumulate_kernel(samples_ref, scaled_ref, top_ref, parts_ref, out_ref, partition_ref, factor_ref):
    partition = merged(parts_ref[...])
    partition_ref[...] = partition
    factor_ref[...] = jnp.exp2(top_ref[...] - partition)
    local = scaled_ref.shape[1]
    sums = jnp.zeros((local, 2 * LANES), jnp.float32)
    ones = jnp.ones((TILE, LANES), jnp.bfloat16)
    for t in range(samples_ref.shape[0] // TILE):
        resp = []
        for h in range(TILE // LANES):
            at = t * (TILE // LANES) + h
            scaled = scaled_ref[at]
            resp.append((scaled * factor_ref[at : at + 1, :]).astype(jnp.bfloat16))
        rows = samples_ref[t * TILE : (t + 1) * TILE, :]
        sums = sums + lax.dot_general(
            jnp.concatenate(resp, axis=1),
            jnp.concatenate([rows, ones], axis=1),
            (((1,), (0,)), ((), ())),
            preferred_element_type=jnp.float32,
        )
    out_ref[0:local, :] = sums[:, :LANES]
    out_ref[local:, :] = jnp.zeros((out_ref.shape[0] - local, LANES), jnp.float32)
    for k in range(local // LANES):
        block = jnp.transpose(sums[k * LANES : (k + 1) * LANES, LANES:])
        out_ref[local + k : local + k + 1, :] = block[0:1, :]


def finish_kernel(denominator, mine_ref, other_ref, centres_ref, new_ref, prior_ref):
    local = centres_ref.shape[0]
    for k in range(local // LANES):
        rows = slice(k * LANES, (k + 1) * LANES)
        at = slice(local + k, local + k + 1)
        mass = mine_ref[at, :] + other_ref[at, :] + 1.0
        prior_ref[k : k + 1, :] = jnp.log(mass / denominator)
        weighted = mine_ref[rows, :] + other_ref[rows, :]
        new_ref[rows, :] = (weighted + centres_ref[rows, :].astype(jnp.float32)) / column_of(mass)


def shared(copies, axis):
    return lax.all_to_all(copies, axis, 0, 0, axis_index_groups=[MEMBERS[axis]], tiled=True)


def on_chip(x):
    return pltpu.with_memory_space_constraint(x, pltpu.VMEM)


def in_hbm(x):
    return pltpu.with_memory_space_constraint(x, pltpu.HBM)


def merged(parts):
    top = jnp.max(parts, axis=0)
    return top + jnp.log2(jnp.sum(jnp.exp2(parts - top), axis=0))


def swapped(x, axis):
    return lax.ppermute(x, axis, [(0, 1), (1, 0)])


def shards(samples, centres, facility_prior_logprob):
    rows, features = samples.shape
    local = centres.shape[0]
    prior = facility_prior_logprob.reshape(local // LANES, LANES)
    lines = rows // LANES
    near, far = "yx", "z"
    whole = pl.BlockSpec(memory_space=pltpu.VMEM)
    copies, samples_here, centres_here, scaled, top = pl.pallas_call(
        stats_kernel,
        in_specs=[pl.BlockSpec(memory_space=pltpu.HBM)] * 3,
        out_specs=[whole] * 5,
        out_shape=(
            pltpu.VMEM((lax.axis_size(near), lines, LANES), jnp.float32),
            pltpu.VMEM((rows, features), samples.dtype),
            pltpu.VMEM((local, features), centres.dtype),
            pltpu.VMEM((lines, local, LANES), jnp.float32),
            pltpu.VMEM((lines, LANES), jnp.float32),
        ),
        compiler_params=SMALL,
        scratch_shapes=[
            pltpu.VMEM(prior.shape, jnp.float32),
            pltpu.VMEM((2, local, TILE), jnp.float32),
            pltpu.SemaphoreType.DMA((CHUNKS + 2,)),
        ],
    )(in_hbm(samples), in_hbm(centres), in_hbm(prior))
    copies = pl.pallas_call(
        merge_kernel,
        in_specs=[whole],
        out_specs=whole,
        out_shape=pltpu.VMEM((lax.axis_size(far), lines, LANES), jnp.float32),
        compiler_params=SMALL,
    )(on_chip(shared(copies, near)))
    parts = shared(copies, far)
    sums, partition = pl.pallas_call(
        accumulate_kernel,
        in_specs=[whole] * 4,
        out_specs=[whole, whole],
        out_shape=(
            pltpu.VMEM((local + 8, features), jnp.float32),
            pltpu.VMEM((lines, LANES), jnp.float32),
        ),
        compiler_params=SMALL,
        scratch_shapes=[pltpu.VMEM((lines, LANES), jnp.float32)],
    )(on_chip(samples_here), on_chip(scaled), on_chip(top), on_chip(parts))
    other = swapped(sums, "xh")
    wide = samples_here.astype(jnp.float32)
    norms = jnp.sum(wide * wide, axis=1)
    log_partition = partition.reshape(rows) * LN2 - norms * inverse_coolness_beta
    sums = sums + other
    other = swapped(sums, "core")
    denominator = float(rows * lax.axis_size(DP) + local * lax.axis_size(CENTRE))
    new_centres, new_log_prior = pl.pallas_call(
        lambda *refs: finish_kernel(denominator, *refs),
        in_specs=[whole, whole, whole],
        out_shape=(
            jax.ShapeDtypeStruct((local, features), jnp.float32),
            jax.ShapeDtypeStruct((local // LANES, LANES), jnp.float32),
        ),
    )(on_chip(sums), on_chip(other), on_chip(centres_here))
    return new_centres, new_log_prior.reshape(local), log_partition


def solution(mesh):
    torus = Mesh(mesh.devices.reshape(2, 2, 8, 8), AXES)
    in_specs = (P(DP, None), P(CENTRE, None), P(CENTRE))
    out_specs = (P(CENTRE, None), P(CENTRE), P(DP))
    return jax.shard_map(
        shards, mesh=torus, in_specs=in_specs, out_specs=out_specs, check_vma=False
    )
```

```python
import jax
import jax.numpy as jnp
import numpy as np
from jax import lax
from jax.experimental import pallas as pl
from jax.experimental.pallas import tpu as pltpu
from jax.sharding import Mesh
from jax.sharding import PartitionSpec as P


AXES = ("xh", "core", "c")
DP = ("xh", "core")
CENTRE = ("c",)
PAIRS = ((4, 5), (3, 2), (7, 6), (1, 0))
ROWS = (2, 3, 1, 0)
MEMBERS = {
    "near": [[8 * z + 2 * y + x for y in ROWS for z in pair] for pair in PAIRS for x in range(2)],
    "far": [[8 * pair[r] + 2 * y + x for pair in PAIRS for x in (1, 0)] for y in range(4) for r in range(2)],
}

inverse_coolness_beta = 0.0625
LOG2E = float(np.log2(np.e))
LN2 = float(np.log(2.0))
CROSS2 = 2.0 * inverse_coolness_beta * LOG2E

LANES = 128
TILE = 256
CHUNKS = 4
ACC = 4
SMALL = pltpu.CompilerParams(vmem_limit_bytes=16 << 20)


def column_of(row):
    return jnp.transpose(jnp.broadcast_to(row, (LANES, LANES)))


def bias_parts(centres_ref, prior_ref):
    wide = centres_ref[...].astype(jnp.float32)
    norm = jnp.sum(wide * wide, axis=1, keepdims=True)
    prior = jnp.concatenate([column_of(prior_ref[k : k + 1, :]) for k in range(prior_ref.shape[0])])
    rest = prior * (0.5 / inverse_coolness_beta) - norm * 0.5
    lane = lax.broadcasted_iota(jnp.int32, rest.shape, 1)
    parts = jnp.zeros(rest.shape, jnp.float32)
    for k in range(3):
        part = rest.astype(jnp.bfloat16).astype(jnp.float32)
        parts = jnp.where(lane == k, part, parts)
        rest = rest - part
    return parts.astype(jnp.bfloat16)


def stats_kernel(
    samples_hbm, centres_hbm, prior_hbm, out_ref, samples_ref, centres_ref, scaled_ref, top_ref, prior_ref, score_ref, sems
):
    pairs = [(centres_hbm, centres_ref), (prior_hbm, prior_ref)]
    step = samples_ref.shape[0] // CHUNKS
    for k in range(CHUNKS):
        rows = pl.ds(k * step, step)
        pairs.append((samples_hbm.at[rows, :], samples_ref.at[rows, :]))
    copies = [pltpu.make_async_copy(a, b, sems.at[k]) for k, (a, b) in enumerate(pairs)]
    for copy in copies:
        copy.start()
    copies[0].wait()
    copies[1].wait()
    extended = jnp.concatenate([centres_ref[...], bias_parts(centres_ref, prior_ref)], axis=1)
    ones = jnp.ones((TILE, LANES), jnp.bfloat16)

    def scores(at):
        rows = samples_ref[at, :]
        return lax.dot_general(
            extended,
            jnp.concatenate([rows, ones[: rows.shape[0], :]], axis=1),
            (((1,), (1,)), ((), ())),
            preferred_element_type=jnp.float32,
        )

    def reduce(t):
        slot = t % 2
        for h in range(TILE // LANES):
            at = t * (TILE // LANES) + h
            lanes = slice(h * LANES, (h + 1) * LANES)
            tops = [score_ref[slot, 8 * r : 8 * r + 8, lanes] for r in range(ACC)]
            for r in range(ACC, local // 8):
                tops[r % ACC] = jnp.maximum(tops[r % ACC], score_ref[slot, 8 * r : 8 * r + 8, lanes])
            while len(tops) > 1:
                tops = [jnp.maximum(a, c) for a, c in zip(tops[::2], tops[1::2])]
            top = jnp.max(tops[0], axis=0, keepdims=True)
            totals = [None] * ACC
            for r in range(local // 8):
                scaled = jnp.exp2((score_ref[slot, 8 * r : 8 * r + 8, lanes] - top) * CROSS2)
                scaled_ref[at, 8 * r : 8 * r + 8, :] = scaled
                totals[r % ACC] = scaled if totals[r % ACC] is None else totals[r % ACC] + scaled
            while len(totals) > 1:
                totals = [a + c for a, c in zip(totals[::2], totals[1::2])]
            total = jnp.sum(totals[0], axis=0, keepdims=True)
            top_ref[at : at + 1, :] = top * CROSS2
            out_ref[0, at : at + 1, :] = top * CROSS2 + jnp.log2(total)

    for copy in copies[2:]:
        copy.wait()
    tiles = samples_ref.shape[0] // TILE
    local = centres_ref.shape[0]
    for h in range(TILE // LANES):
        lanes = slice(h * LANES, (h + 1) * LANES)
        score_ref[0, :, lanes] = scores(lanes)
    for t in range(tiles):
        if t + 1 < tiles:
            score_ref[(t + 1) % 2, :, :] = scores(slice((t + 1) * TILE, (t + 2) * TILE))
        reduce(t)
    for k in range(1, out_ref.shape[0]):
        out_ref[k, :, :] = out_ref[0, :, :]


def merge_kernel(parts_ref, out_ref):
    part = merged(parts_ref[...])
    for k in range(out_ref.shape[0]):
        out_ref[k, :, :] = part


def accumulate_kernel(samples_ref, scaled_ref, top_ref, parts_ref, out_ref, partition_ref, factor_ref):
    partition = merged(parts_ref[...])
    partition_ref[...] = partition
    factor_ref[...] = jnp.exp2(top_ref[...] - partition)
    local = scaled_ref.shape[1]
    sums = jnp.zeros((local, 2 * LANES), jnp.float32)
    ones = jnp.ones((TILE, LANES), jnp.bfloat16)
    for t in range(samples_ref.shape[0] // TILE):
        resp = []
        for h in range(TILE // LANES):
            at = t * (TILE // LANES) + h
            scaled = scaled_ref[at]
            resp.append((scaled * factor_ref[at : at + 1, :]).astype(jnp.bfloat16))
        rows = samples_ref[t * TILE : (t + 1) * TILE, :]
        sums = sums + lax.dot_general(
            jnp.concatenate(resp, axis=1),
            jnp.concatenate([rows, ones], axis=1),
            (((1,), (0,)), ((), ())),
            preferred_element_type=jnp.float32,
        )
    out_ref[0:local, :] = sums[:, :LANES]
    out_ref[local:, :] = jnp.zeros((out_ref.shape[0] - local, LANES), jnp.float32)
    for k in range(local // LANES):
        block = jnp.transpose(sums[k * LANES : (k + 1) * LANES, LANES:])
        out_ref[local + k : local + k + 1, :] = block[0:1, :]


def finish_kernel(denominator, mine_ref, other_ref, centres_ref, new_ref, prior_ref):
    local = centres_ref.shape[0]
    for k in range(local // LANES):
        rows = slice(k * LANES, (k + 1) * LANES)
        at = slice(local + k, local + k + 1)
        mass = mine_ref[at, :] + other_ref[at, :] + 1.0
        prior_ref[k : k + 1, :] = jnp.log(mass / denominator)
        weighted = mine_ref[rows, :] + other_ref[rows, :]
        new_ref[rows, :] = (weighted + centres_ref[rows, :].astype(jnp.float32)) / column_of(mass)


def shared(copies, axis):
    return lax.all_to_all(copies, "c", 0, 0, axis_index_groups=MEMBERS[axis], tiled=True)


def on_chip(x):
    return pltpu.with_memory_space_constraint(x, pltpu.VMEM)


def in_hbm(x):
    return pltpu.with_memory_space_constraint(x, pltpu.HBM)


def merged(parts):
    top = jnp.max(parts, axis=0)
    return top + jnp.log2(jnp.sum(jnp.exp2(parts - top), axis=0))


def swapped(x, axis):
    return lax.ppermute(x, axis, [(0, 1), (1, 0)])


def shards(samples, centres, facility_prior_logprob):
    rows, features = samples.shape
    local = centres.shape[0]
    prior = facility_prior_logprob.reshape(local // LANES, LANES)
    lines = rows // LANES
    near, far = "near", "far"
    whole = pl.BlockSpec(memory_space=pltpu.VMEM)
    copies, samples_here, centres_here, scaled, top = pl.pallas_call(
        stats_kernel,
        in_specs=[pl.BlockSpec(memory_space=pltpu.HBM)] * 3,
        out_specs=[whole] * 5,
        out_shape=(
            pltpu.VMEM((len(MEMBERS[near][0]), lines, LANES), jnp.float32),
            pltpu.VMEM((rows, features), samples.dtype),
            pltpu.VMEM((local, features), centres.dtype),
            pltpu.VMEM((lines, local, LANES), jnp.float32),
            pltpu.VMEM((lines, LANES), jnp.float32),
        ),
        compiler_params=SMALL,
        scratch_shapes=[
            pltpu.VMEM(prior.shape, jnp.float32),
            pltpu.VMEM((2, local, TILE), jnp.float32),
            pltpu.SemaphoreType.DMA((CHUNKS + 2,)),
        ],
    )(in_hbm(samples), in_hbm(centres), in_hbm(prior))
    copies = pl.pallas_call(
        merge_kernel,
        in_specs=[whole],
        out_specs=whole,
        out_shape=pltpu.VMEM((len(MEMBERS[far][0]), lines, LANES), jnp.float32),
        compiler_params=SMALL,
    )(on_chip(shared(copies, near)))
    parts = shared(copies, far)
    sums, partition = pl.pallas_call(
        accumulate_kernel,
        in_specs=[whole] * 4,
        out_specs=[whole, whole],
        out_shape=(
            pltpu.VMEM((local + 8, features), jnp.float32),
            pltpu.VMEM((lines, LANES), jnp.float32),
        ),
        compiler_params=SMALL,
        scratch_shapes=[pltpu.VMEM((lines, LANES), jnp.float32)],
    )(on_chip(samples_here), on_chip(scaled), on_chip(top), on_chip(parts))
    other = swapped(sums, "xh")
    wide = samples_here.astype(jnp.float32)
    norms = jnp.sum(wide * wide, axis=1)
    log_partition = partition.reshape(rows) * LN2 - norms * inverse_coolness_beta
    sums = sums + other
    other = swapped(sums, "core")
    denominator = float(rows * lax.axis_size(DP) + local * lax.axis_size(CENTRE))
    new_centres, new_log_prior = pl.pallas_call(
        lambda *refs: finish_kernel(denominator, *refs),
        in_specs=[whole, whole, whole],
        out_shape=(
            jax.ShapeDtypeStruct((local, features), jnp.float32),
            jax.ShapeDtypeStruct((local // LANES, LANES), jnp.float32),
        ),
    )(on_chip(sums), on_chip(other), on_chip(centres_here))
    return new_centres, new_log_prior.reshape(local), log_partition


def solution(mesh):
    torus = Mesh(mesh.devices.reshape(2, 2, 64), AXES)
    in_specs = (P(DP, None), P(CENTRE, None), P(CENTRE))
    out_specs = (P(CENTRE, None), P(CENTRE), P(DP))
    return jax.shard_map(
        shards, mesh=torus, in_specs=in_specs, out_specs=out_specs, check_vma=False
    )
```
